768 devices in a mesh: dp: 16 (over x, z_lo), expert: 8 (over y), tensor: 6 (over z_hi, core).
Axes of the slice: x: 4, y: 8, z: 12 (z_hi: 3, z_lo: 4; z = z_hi * 4 + z_lo), core: 2. Of those that a mesh axis runs over, the one named last changes fastest.
Arguments:
- tokens: bfloat16 [2048, 6144], P('dp'), may hold values from -6 to 6
- norm_gain: float32 [6144], replicated, may hold values from 0.1 to 1.9
- expert_ids: int32 [2048, 2], P('dp'), may hold values from 0 to 7, all different within a row; in each aligned block of 128 rows (0 to 127, 128 to 255, ...) at most 36 rows name the same one
- gate_weights: float32 [2048, 2], P('dp'), may hold values from 0.1 to 0.9
- w_gate: bfloat16 [8, 6144, 12288], P('expert', None, ('dp', 'tensor')), may hold values from -0.078125 to 0.078125
- w_up: bfloat16 [8, 6144, 12288], P('expert', None, ('dp', 'tensor')), may hold values from -0.078125 to 0.078125
- w_down: bfloat16 [8, 12288, 6144], P('expert', 'dp', 'tensor'), may hold values from -0.0546875 to 0.0546875
- label_rows: bfloat16 [2048, 6144], P(('dp', 'expert'), 'tensor'), may hold values from -4 to 4, as said below
- seg_ids: int32 [16, 128], P('dp'), may hold values from 0 to 3, never falling along the last dimension, each value on 1 to 64 neighbouring positions
- pair_slot: int32 [16, 4], P('dp'), may hold values from 0 to 3, each once within a row
- ref_scores: float32 [16, 4], P('dp'), may hold values from -8 to 8
Outputs:
- layer_out: bfloat16 [2048, 6144], P(('dp', 'expert'), 'tensor')
- margins: float32 [16, 2], P('dp')
The draws below stay inside these ranges and needn't reach their ends.
Inputs may be any that keep to these rules, and one draw needn't show every extreme that they name: `expert_ids`: each row names two different experts. Among the 128 rows of one dp group no expert is named more than 36 times, and in some group some expert is named exactly 36 times. `seg_ids`: within each row sequence numbers never fall; every sequence has 1 to 64 tokens and one has exactly 64. `pair_slot`: each row holds every number of 0 to 3 once. `label_rows`: entries lie within 27 / sqrt(6144) in magnitude.
All inputs are finite; a program needn't handle non-finite values.
Results may differ from the reference program's by a relative error of at most 0.009.
Values may be sent and summed in bfloat16 or wider, within the bound.
No kernel may reach another device: no remote copies, remote signals or barrier semaphores. Data moves between devices by JAX's collectives and lax.ppermute only.
A program may use at most 64 MiB of HBM per device.

```python
import math
from functools import partial
import jax
import jax.numpy as jnp
import numpy as np
from jax import lax

D = 6144
FF = 12288
EXPERTS = 8
TOK_GROUP = 128
CAP = 36
TOKENS = 2048
DPG = 16
SEQS = 4
PAIRS = 2
SEQ_MOST = 64
N_DP = 16


def draw_label_rows(key, part):
    row_pos = jnp.arange(TOKENS, dtype=jnp.float32)
    col_pos = jnp.arange(D, dtype=jnp.float32)
    row_rise = 1.0 + 2.0 * jnp.mod(row_pos, TOK_GROUP) / TOK_GROUP
    col_rise = 1.0 + 2.0 * col_pos / D
    base = jnp.clip(jax.random.normal(key, (TOKENS, D), jnp.float32), -6.0, 6.0)
    factor = 0.5 * row_rise[:, None] * col_rise[None, :]
    return (base * factor / math.sqrt(D)).astype(jnp.bfloat16)


def shard_levels(own_key, extent, cuts, least, high):
    loudness = 1.0
    for dim, parts in cuts:
        heights = jax.random.uniform(jax.random.fold_in(jax.random.fold_in(own_key, 6), dim), (parts,), jnp.float32, least / len(cuts), high / len(cuts))
        loudness = loudness * jnp.repeat(jnp.exp(heights), extent[dim] // parts).reshape((-1,) + (1,) * (len(extent) - 1 - dim))
    return loudness


def split_up(amount, total, most, slope):
    weights = [(1 << 20) // math.isqrt(standing ** slope) + 1 for standing in range(2, amount + 1)]
    rest, holding = total - most - (amount - 1), [1] * (amount - 1)
    while rest > 0:
        movable = [i for i in range(amount - 1) if holding[i] < most]
        mass, left = sum([weights[i] for i in movable]), rest
        for i in movable:
            extra = min(most - holding[i], max(1, left * weights[i] // mass), rest)
            holding[i] = holding[i] + extra
            rest = rest - extra
    return np.array([most] + holding)


def ragged_sizes(own_key, number_of, total, bound, slope):
    if number_of == 2:
        one = jax.random.randint(own_key, (), max(1, total - bound), min(bound, total - 1) + 1)
        return jnp.stack([one, total - one])
    tallies = jnp.asarray(split_up(number_of, total, bound, slope), jnp.int32)
    pairs = (number_of - 1) // 2
    giver, taker = tallies[1:1 + 2 * pairs:2], tallies[2:2 + 2 * pairs:2]
    margin = jnp.minimum(giver - 1, bound - taker)
    passed = jax.random.randint(jax.random.fold_in(own_key, 1), (pairs,), 0, 1 << 20) % (margin + 1)
    tallies = tallies.at[1:1 + 2 * pairs:2].set(giver - passed).at[2:2 + 2 * pairs:2].set(taker + passed)
    return tallies[jax.random.permutation(jax.random.fold_in(own_key, 2), number_of)]


def shared_out(key, own, number, rows, count, top, reach, slope):
    ranking = jax.random.permutation(key, count)
    heavy_load, common = shares(count, rows * top, reach, slope, True), shares(count, rows * top, reach, slope, False)
    places = jnp.arange(count)

    def named(tallies, rotation):
        used = int((tallies > 0).sum())
        fixed = max(1, used // 4)
        shifted = fixed + (places - fixed + rotation * (used - fixed)) % max(1, count - fixed)
        return jnp.zeros((count,), jnp.int32).at[ranking[jnp.where(places < fixed, places, shifted)]].set(jnp.asarray(tallies, jnp.int32))

    tallies = jnp.where(number % 4 == 0, named(heavy_load, number // 4), named(common, number - number // 4 - 1))
    mixed = jax.random.permutation(jax.random.fold_in(own, 3), count)
    source_of, receiver = mixed[0:count // 2 * 2:2], mixed[1:count // 2 * 2:2]
    room = jnp.minimum(tallies[source_of] - 1, reach - tallies[receiver]) // 2
    room = jnp.where((source_of == ranking[0]) | (receiver == ranking[0]) | (tallies[receiver] == 0), 0, jnp.maximum(room, 0))
    shifted = jax.random.randint(jax.random.fold_in(own, 4), (count // 2,), 0, 1 << 20) % (room + 1)
    tallies = tallies.at[source_of].add(-shifted).at[receiver].add(shifted)
    labels = jnp.searchsorted(jnp.cumsum(tallies), jnp.arange(rows * top), side="right").astype(jnp.int32)
    table = labels.reshape(top, rows).T
    table = table[jax.random.permutation(jax.random.fold_in(own, 1), rows)]
    rotation = jax.random.randint(jax.random.fold_in(own, 2), (rows, 1), 0, top)
    return jnp.take_along_axis(table, (jnp.arange(top)[None, :] + rotation) % top, axis=1)


def shares(number_of, total, limit, lean, full):
    weights = [(1 << 20) // math.isqrt(grade ** lean) + 1 for grade in range(1, number_of + 1)]
    largest = limit if full else min(limit, max(-(-total // number_of), total * weights[0] // sum(weights)))
    least = 1 if total - largest >= number_of - 1 else 0
    holding, rest = [largest] + [least] * (number_of - 1), total - largest - least * (number_of - 1)
    while rest > 0:
        candidates = [i for i in range(1, number_of) if holding[i] < largest] or [i for i in range(1, number_of) if holding[i] < limit]
        mass, left = sum([weights[i] for i in candidates]), rest
        for i in candidates:
            more = min(limit - holding[i], max(1, left * weights[i] // mass), rest)
            holding[i] = holding[i] + more
            rest = rest - more
    return np.array(holding)


def bell_draw(key, shape, width, reach, split=(), held_as=jnp.bfloat16):
    result = width * jax.random.normal(key, shape, jnp.float32)
    if split:
        result = result * shard_levels(key, shape, split, -0.22, 0.18)
    return jnp.clip(result, -reach, reach).astype(held_as)


def setup_inputs(seed: int = 0) -> dict:
    keys = jax.random.split(jax.random.key(seed), 12)
    tokens = bell_draw(keys[0], (TOKENS, D), 1.0, 6.0, ((0, 16),))
    norm_gain = jnp.clip(1.0 + 0.18 * jax.random.normal(keys[1], (D,), jnp.float32), 0.1, 1.9)
    expert_ids_keys = jax.random.split(jax.random.fold_in(keys[2], 1), TOKENS // TOK_GROUP)
    expert_ids_turns = jax.random.permutation(jax.random.fold_in(keys[2], 3), TOKENS // TOK_GROUP)
    expert_ids = jax.vmap(lambda own, number: shared_out(jax.random.fold_in(keys[2], 2), own, number, TOK_GROUP, EXPERTS, 2, CAP, 2))(expert_ids_keys, expert_ids_turns).reshape((TOKENS, 2))
    gate_weights = jnp.clip(0.1 + 0.79999997 * jax.random.uniform(keys[3], (TOKENS, 2), jnp.float32) ** shard_levels(keys[3], (TOKENS, 2), ((0, 16),), -0.2, 0.2), 0.1, 0.9)
    w_gate = bell_draw(keys[4], (EXPERTS, D, FF), D ** -0.5, 0.078125, ((0, 8), (2, 96)))
    w_up = bell_draw(keys[5], (EXPERTS, D, FF), D ** -0.5, 0.078125, ((0, 8), (2, 96)))
    w_down = bell_draw(keys[6], (EXPERTS, FF, D), FF ** -0.5, 0.0546875, ((0, 8), (1, 16), (2, 6)))
    label_rows = draw_label_rows(jax.random.fold_in(keys[11], 71), 0)
    seg_ids = jax.vmap(lambda own: jnp.searchsorted(jnp.cumsum(ragged_sizes(own, SEQS, TOK_GROUP, SEQ_MOST, 1)), jnp.arange(TOK_GROUP), side="right"))(jax.random.split(keys[8], DPG)).reshape((DPG, TOK_GROUP)).astype(jnp.int32)
    pair_slot = jax.vmap(lambda own: jax.random.permutation(own, SEQS))(jax.random.split(keys[9], DPG)).reshape((DPG, SEQS)).astype(jnp.int32)
    ref_scores = bell_draw(keys[10], (DPG, SEQS), 2.0, 8.0, ((0, 16),), jnp.float32)
    return {"tokens": tokens, "norm_gain": norm_gain, "expert_ids": expert_ids, "gate_weights": gate_weights, "w_gate": w_gate, "w_up": w_up, "w_down": w_down, "label_rows": label_rows, "seg_ids": seg_ids, "pair_slot": pair_slot, "ref_scores": ref_scores}


epsilon = 1e-05
dpo_beta = 0.5

def normed_rows(tokens, norm_gain):
    values = tokens.astype(jnp.float32)
    inverse_rms = lax.rsqrt(lax.optimization_barrier(jnp.mean(values * values, axis=1, keepdims=True)) + epsilon)
    return (values * inverse_rms * norm_gain[None, :].astype(jnp.float32)).astype(jnp.bfloat16)

def slot_tables(expert_ids, gate_weights, experts, capacity):
    tok_count = expert_ids.shape[0]
    flat_ids = expert_ids.reshape(-1).astype(jnp.int32)
    onehot = (flat_ids[:, None] == jnp.arange(experts, dtype=jnp.int32)[None, :]).astype(jnp.int32)
    earlier = jnp.cumsum(onehot, axis=0).astype(jnp.int32) - onehot
    position = lax.optimization_barrier(jnp.sum(earlier * onehot, axis=1)).astype(jnp.int32)
    slot_index = flat_ids * capacity + position
    slot_match = (slot_index[:, None] == jnp.arange(experts * capacity, dtype=jnp.int32)[None, :]).astype(jnp.float32)
    slot_match = slot_match.reshape(tok_count, 2, experts * capacity)
    placement = lax.optimization_barrier(jnp.sum(slot_match, axis=1))
    mixing = lax.optimization_barrier(jnp.sum(slot_match * gate_weights[:, :, None].astype(jnp.float32), axis=1))
    return (placement, mixing)

def rounded_term(value):
    narrow = lax.optimization_barrier(value.astype(jnp.bfloat16))
    return narrow.astype(jnp.float32)

def run_expert(operands):
    rows, gate_matrix, up_matrix, down_matrix = operands
    gate_sum = jnp.dot(rows, gate_matrix, preferred_element_type=jnp.float32)
    up_sum = jnp.dot(rows, up_matrix, preferred_element_type=jnp.float32)
    hidden = (jax.nn.silu(gate_sum) * up_sum).astype(jnp.bfloat16)
    block = FF // N_DP
    total = jnp.zeros((rows.shape[0], down_matrix.shape[1]), jnp.float32)
    for index in range(N_DP):
        piece = jnp.dot(hidden[:, index * block:(index + 1) * block], down_matrix[index * block:(index + 1) * block], preferred_element_type=jnp.float32)
        total = total + rounded_term(piece)
    return total.astype(jnp.bfloat16)

def reference(tokens, norm_gain, expert_ids, gate_weights, w_gate, w_up, w_down, label_rows, seg_ids, pair_slot, ref_scores):
    groups = N_DP
    normed = normed_rows(tokens, norm_gain).reshape(groups, TOK_GROUP, D)
    tables = partial(slot_tables, experts=EXPERTS, capacity=CAP)
    placement, mixing = jax.vmap(tables)(expert_ids.reshape(groups, TOK_GROUP, 2), gate_weights.reshape(groups, TOK_GROUP, 2))
    outgoing = jnp.einsum('gts,gtd->gsd', placement.astype(jnp.float32), normed.astype(jnp.float32)).astype(jnp.bfloat16)
    by_expert = outgoing.reshape(groups, EXPERTS, CAP, D).transpose(1, 0, 2, 3).reshape(EXPERTS, groups * CAP, D)
    expert_out = lax.map(run_expert, (by_expert, w_gate, w_up, w_down))
    per_expert = expert_out.reshape(EXPERTS, groups, CAP, D)
    mixing_parts = mixing.reshape(groups, TOK_GROUP, EXPERTS, CAP)
    expert_mix = jnp.zeros((groups, TOK_GROUP, D), jnp.float32)
    for expert in range(EXPERTS):
        term = jnp.einsum('gtc,gcd->gtd', mixing_parts[:, :, expert, :], per_expert[expert].astype(jnp.float32), precision=lax.Precision.HIGHEST)
        expert_mix = expert_mix + rounded_term(term)
    mixed = tokens.astype(jnp.float32) + expert_mix.reshape(TOKENS, D)
    layer_out = mixed.astype(jnp.bfloat16)
    token_score = lax.optimization_barrier(jnp.sum(mixed * label_rows.astype(jnp.float32), axis=1)).reshape(N_DP, TOK_GROUP)
    member = (seg_ids[:, :, None] == jnp.arange(SEQS, dtype=jnp.int32)[None, None, :]).astype(jnp.float32)
    totals = lax.optimization_barrier(jnp.sum(member * token_score[:, :, None], axis=1))
    polarity = (1 - 2 * (pair_slot % 2)).astype(jnp.float32)
    pair_member = ((pair_slot // 2)[:, :, None] == jnp.arange(PAIRS, dtype=jnp.int32)[None, None, :]).astype(jnp.float32)
    margins = dpo_beta * lax.optimization_barrier(jnp.sum(pair_member * (polarity * (totals - ref_scores))[:, :, None], axis=1))
    return (layer_out, margins)
```

```python
import jax
import jax.numpy as jnp
from jax import lax
from jax.sharding import Mesh, PartitionSpec as P

SEQS = 4
PAIRS = 2
CAP = 36
epsilon = 1e-05
dpo_beta = 0.5

AXES = ("x", "zl", "y", "zh", "c")
DP = ("x", "zl")
TENSOR = ("zh", "c")


def shift_pairs(sizes, dz=0, dc=0):
    nx, nl, ny, nh, nc = sizes
    nz = nh * nl

    def flat(x, y, z, c):
        return (((x * nl + z % nl) * ny + y) * nh + z // nl) * nc + c

    return [
        (flat(x, y, z, c), flat(x, y, (z + dz) % nz, (c + dc) % nc))
        for x in range(nx)
        for y in range(ny)
        for z in range(nz)
        for c in range(nc)
    ]


def exchange(array, axis):
    return lax.all_to_all(array, axis, 0, 0, tiled=True)


def for_each(array, count):
    return jnp.broadcast_to(array[None], (count, *array.shape))


def make_body(sizes):
    nx, nl, ny, nh, nc = sizes

    def shifted(array, dz=0, dc=0):
        return lax.ppermute(array, AXES, shift_pairs(sizes, dz, dc))

    def body(
        tokens,
        norm_gain,
        expert_ids,
        gate_weights,
        w_gate,
        w_up,
        w_down,
        label_rows,
        seg_ids,
        pair_slot,
        ref_scores,
    ):
        count, width = tokens.shape
        expert = lax.axis_index("y")
        zl = lax.axis_index("zl")
        zh = lax.axis_index("zh")
        core = lax.axis_index("c")
        half = width // nc
        columns = width // (nh * nc)
        own_count = count // ny
        values = tokens.astype(jnp.float32)
        inverse_rms = lax.rsqrt(
            jnp.mean(values * values, axis=1, keepdims=True) + epsilon
        )
        my_values = lax.dynamic_slice_in_dim(tokens, core * half, half, 1).astype(
            jnp.float32
        )
        my_gain = lax.dynamic_slice_in_dim(norm_gain, core * half, half, 0)
        normed = (my_values * inverse_rms * my_gain[None, :]).astype(jnp.bfloat16)
        ids = expert_ids.T
        weights = gate_weights.T
        match = ids == expert
        named = jnp.any(match, axis=0)
        gate = jnp.sum(jnp.where(match, weights, 0.0), axis=0)
        earlier = jnp.arange(count)[:, None] < jnp.arange(count)[None, :]
        position = jnp.sum(
            jnp.where(earlier & named[:, None], 1, 0), axis=0, dtype=jnp.int32
        )
        place = (
            (position[None, :] == jnp.arange(CAP, dtype=jnp.int32)[:, None])
            & named[None, :]
        ).astype(jnp.bfloat16)
        own = jnp.dot(place, normed, preferred_element_type=jnp.float32).astype(
            jnp.bfloat16
        )
        part = half // 2
        far_a = shifted(own[:, :part], dz=2)
        far_b = shifted(own[:, part:], dz=-2)
        near = exchange(for_each(own, nx), "x").reshape(nx * CAP, half)
        below = shifted(near, dz=1)
        above = shifted(near, dz=-1)
        far = jnp.concatenate([far_a, far_b], axis=1)
        far = exchange(for_each(far, nx), "x").reshape(nx * CAP, half)
        w_both = jnp.concatenate([w_gate[0], w_up[0]], axis=1)
        w_mine = lax.dynamic_slice_in_dim(w_both, core * half, half, 0)
        w_other = shifted(
            lax.dynamic_slice_in_dim(w_both, (1 - core) * half, half, 0), dc=1
        )
        rows = [near, below, above, far]

        def partial_sum(weights):
            return jnp.concatenate(
                [
                    jnp.dot(r, weights, preferred_element_type=jnp.float32)
                    for r in rows
                ],
                axis=0,
            )

        theirs = shifted(partial_sum(w_other), dc=1)
        sums = partial_sum(w_mine) + theirs
        units = sums.shape[1] // 2
        hidden = (jax.nn.silu(sums[:, :units]) * sums[:, units:]).astype(jnp.bfloat16)
        before = shifted(hidden, dz=nl)
        after = shifted(hidden, dz=-nl)
        mine = jnp.stack([hidden, after, before])
        others = shifted(mine, dc=1)
        low = jnp.where(core == 0, mine, others)
        high = jnp.where(core == 0, others, mine)
        down = w_down[0].reshape(nh, 2 * units, columns)
        total = 0.0
        for step in range(nh):
            block = jnp.concatenate([low[step], high[step]], axis=1)
            total = total + jnp.dot(
                block,
                lax.dynamic_index_in_dim(down, (zh + step) % nh, 0, keepdims=False),
                preferred_element_type=jnp.float32,
            )
        down_part = total.astype(jnp.bfloat16).reshape(4, nx, CAP, columns)
        by_x = jnp.moveaxis(down_part, 1, 0)
        over_x = jnp.sum(exchange(by_x, "x").astype(jnp.float32), axis=0).astype(
            jnp.bfloat16
        )
        by_offset = jnp.stack([over_x[0], over_x[2], over_x[3], over_x[1]])
        order = (jnp.arange(nl) - zl) % nl
        by_zl = jnp.take(by_offset, order, axis=0)
        own_rows = jnp.sum(exchange(by_zl, "zl").astype(jnp.float32), axis=0).astype(
            jnp.bfloat16
        )
        picked = lax.dot_general(
            place,
            own_rows,
            (((0,), (0,)), ((), ())),
            preferred_element_type=jnp.float32,
        )
        weighted = (gate[:, None] * picked).astype(jnp.bfloat16)
        terms = exchange(weighted.reshape(ny, own_count, columns), "y")
        expert_mix = jnp.sum(terms.astype(jnp.float32), axis=0)
        tensor_index = zh * nc + core
        residual = lax.dynamic_slice(
            tokens,
            (expert * own_count, tensor_index * columns),
            (own_count, columns),
        ).astype(jnp.float32)
        mixed = residual + expert_mix
        layer_out = mixed.astype(jnp.bfloat16)
        token_score = jnp.sum(mixed * label_rows.astype(jnp.float32), axis=1)
        sequence_ids = lax.dynamic_slice_in_dim(
            seg_ids[0], expert * own_count, own_count, 0
        )
        member = (
            sequence_ids[:, None] == jnp.arange(SEQS, dtype=jnp.int32)[None, :]
        ).astype(jnp.float32)
        partial_value = jnp.sum(member * token_score[:, None], axis=0)
        totals = exchange(
            for_each(partial_value[None], ny * nh * nc), ("y", "zh", "c")
        ).sum(axis=(0, 1))
        slots_here = pair_slot[0]
        polarity = (1 - 2 * (slots_here % 2)).astype(jnp.float32)
        pair_member = (
            (slots_here // 2)[:, None] == jnp.arange(PAIRS, dtype=jnp.int32)[None, :]
        ).astype(jnp.float32)
        margins = dpo_beta * jnp.sum(
            pair_member * (polarity * (totals - ref_scores[0]))[:, None], axis=0
        )
        return (layer_out, margins[None, :])

    return body


def solution(mesh):
    sizes = (4, 4, mesh.shape["expert"], 3, 2)
    fine = Mesh(mesh.devices.reshape(sizes), AXES)
    placed = (
        P(DP, None),
        P(),
        P(DP, None),
        P(DP, None),
        P("y", None, (*DP, *TENSOR)),
        P("y", None, (*DP, *TENSOR)),
        P("y", DP, TENSOR),
        P((*DP, "y"), TENSOR),
        P(DP, None),
        P(DP, None),
        P(DP, None),
    )
    return jax.shard_map(
        make_body(sizes),
        mesh=fine,
        in_specs=placed,
        out_specs=(P((*DP, "y"), TENSOR), P(DP, None)),
        check_vma=False,
    )
```

```python
import functools

import jax
import jax.numpy as jnp
from jax import lax
from jax.experimental import pallas as pl
from jax.experimental.pallas import tpu as pltpu
from jax.sharding import Mesh, PartitionSpec as P

SEQS = 4
PAIRS = 2
SLOTS = 40
LANES = 128
epsilon = 1e-05
dpo_beta = 0.5

AXES = ("x", "zl", "y", "zh", "c")
DP = ("x", "zl")
TENSOR = ("zh", "c")
OFFSETS = (0, 2, -1, 1)


f32 = jnp.float32
bf16 = jnp.bfloat16
VMEM = pl.BlockSpec(memory_space=pltpu.VMEM)
ANY = pl.BlockSpec(memory_space=pl.ANY)


def shift_pairs(sizes, dz=0, dc=0):
    nx, nl, ny, nh, nc = sizes
    nz = nh * nl

    def flat(x, y, z, c):
        return (((x * nl + z % nl) * ny + y) * nh + z // nl) * nc + c

    return [
        (flat(x, y, z, c), flat(x, y, (z + dz) % nz, (c + dc) % nc))
        for x in range(nx)
        for y in range(ny)
        for z in range(nz)
        for c in range(nc)
    ]


def exchange(array, axis):
    return lax.all_to_all(array, axis, 0, 0, tiled=True)


def for_each(array, count):
    return jnp.broadcast_to(array[None], (count, *array.shape))


def call(kernel, outs, ins, flops=0, in_specs=None, scratch=(), spare=4):
    size = sum(a.size * a.dtype.itemsize for a in (*ins, *outs))
    limit = min(size + (spare << 20), 60 << 20)
    return pl.pallas_call(
        kernel,
        out_shape=outs,
        in_specs=in_specs or [VMEM] * len(ins),
        out_specs=tuple(VMEM for _ in outs),
        scratch_shapes=list(scratch),
        compiler_params=pltpu.CompilerParams(vmem_limit_bytes=limit),
        cost_estimate=pl.CostEstimate(
            flops=flops or size, bytes_accessed=size, transcendentals=0
        ),
    )(*ins)


def column(row):
    return jnp.transpose(jnp.broadcast_to(row, (LANES, LANES)))


def front_kernel(own_count, columns, tok_ref, gain_ref, ids_ref, gw_ref, near_ref, far_ref, place_ref, gate_ref, res_ref):
    count, width = tok_ref.shape
    half = near_ref.shape[2]
    expert = lax.axis_index("y")
    core = lax.axis_index("c")
    step = 512
    squares = jnp.zeros((count, step), f32)
    for start in range(0, width, step):
        v = tok_ref[:, start : start + step].astype(f32)
        squares = squares + v * v
    total = jnp.sum(squares, axis=1, keepdims=True)
    inverse_rms = lax.rsqrt(total * (1.0 / width) + epsilon)
    match = ids_ref[...] == expert
    hit = match.astype(f32)
    named = hit[0:1] + hit[1:2]
    gate_row = jnp.sum(jnp.where(match, gw_ref[...], 0.0), axis=0, keepdims=True)
    gate_ref[...] = column(gate_row)
    before = lax.broadcasted_iota(jnp.int32, (count, count), 0)
    after = lax.broadcasted_iota(jnp.int32, (count, count), 1)
    position = jnp.dot(
        jnp.broadcast_to(named, (8, count)).astype(bf16),
        (before < after).astype(bf16),
        preferred_element_type=f32,
    )[0:1]
    slot = lax.broadcasted_iota(jnp.int32, (SLOTS, count), 0).astype(f32)
    place = jnp.where((slot == position) & (named > 0.5), 1.0, 0.0).astype(bf16)
    place_ref[...] = place
    nc = width // half
    column_at = (lax.axis_index("zh") * nc + core) * columns
    res_ref[...] = tok_ref[
        pl.ds(pl.multiple_of(expert * own_count, own_count), own_count),
        pl.ds(pl.multiple_of(column_at, LANES), columns),
    ]
    for start in range(0, half, step):
        at = pl.multiple_of(core * half + start, LANES)
        v = tok_ref[:, pl.ds(at, step)].astype(f32)
        normed = (v * inverse_rms * gain_ref[:, pl.ds(at, step)]).astype(bf16)
        rows = jnp.dot(place, normed, preferred_element_type=f32).astype(bf16)
        for x in range(near_ref.shape[0]):
            near_ref[x, :, start : start + step] = rows
        far_ref[:, start : start + step] = rows


def far_kernel(in_ref, out_ref):
    for x in range(out_ref.shape[0]):
        out_ref[x] = in_ref[...]


def slice_kernel(gate_ref, up_ref, send_ref, keep_ref, sems):
    half = send_ref.shape[1]
    core = lax.axis_index("c")
    copies = []
    for i, ref in enumerate((gate_ref, up_ref)):
        for j, (out, c) in enumerate(((send_ref, 1 - core), (keep_ref, core))):
            at = pl.multiple_of(c * half, 8)
            copies.append(
                pltpu.make_async_copy(
                    ref.at[0, pl.ds(at, half)], out.at[i], sems.at[2 * i + j]
                )
            )
    for copy in copies:
        copy.start()
    for copy in copies:
        copy.wait()


def dots_kernel(a_ref, b_ref, w_ref, *refs):
    *first, out_ref, sum_ref = refs
    _, half = a_ref.shape
    step = 512
    sum_ref[...] = jnp.zeros_like(sum_ref)

    def body(k, _):
        at = pl.multiple_of(k * step, step)
        x = jnp.concatenate(
            [a_ref[:, pl.ds(at, step)], b_ref[:, pl.ds(at, step)]], axis=0
        )
        w = jnp.concatenate(
            [w_ref[0, pl.ds(at, step), :], w_ref[1, pl.ds(at, step), :]], axis=1
        )
        sum_ref[...] += jnp.dot(x, w, preferred_element_type=f32)
        return 0

    lax.fori_loop(0, half // step, body, 0)
    at = 0
    for ref in first:
        out_ref[at : at + ref.shape[0]] = ref[...]
        at += ref.shape[0]
    out_ref[at:] = sum_ref[...]


def dots(a, b, w, *first):
    rows, half = a.shape
    wide = 2 * w.shape[2]
    out = jax.ShapeDtypeStruct((2 * rows + sum(p.shape[0] for p in first), wide), f32)
    (sums,) = call(
        dots_kernel,
        (out,),
        (a, b, w, *first),
        flops=2 * 2 * rows * half * wide,
        scratch=[pltpu.VMEM((2 * rows, wide), f32)],
    )
    return sums


def hidden_kernel(mine_ref, theirs_ref, out_ref):
    nx, nl, slots, units = out_ref.shape
    zl = lax.axis_index("zl")
    for r, offset in enumerate(OFFSETS):
        to = lax.rem(zl + offset + nl, nl)
        for x in range(nx):
            at = (r * nx + x) * slots
            sums = mine_ref[at : at + slots] + theirs_ref[at : at + slots]
            gate, up = sums[:, :units], sums[:, units:]
            out_ref[x, to] = (gate / (1.0 + jnp.exp(-gate)) * up).astype(bf16)


def stack_kernel(a_ref, b_ref, c_ref, out_ref):
    for i, ref in enumerate((a_ref, b_ref, c_ref)):
        out_ref[i] = ref[...]


def down_kernel(nh, mine_ref, other_ref, w_ref, out_ref):
    nx, rows, _ = out_ref.shape
    units = mine_ref.shape[2]
    zh = lax.axis_index("zh")
    core = lax.axis_index("c")
    weights = []
    for step in range(nh):
        base = lax.rem(zh + step, nh) * 2
        weights.append(
            jnp.concatenate(
                [
                    w_ref[0, pl.ds(pl.multiple_of((base + c) * units, units), units), :]
                    for c in (core, 1 - core)
                ],
                axis=0,
            )
        )
    for x in range(nx):
        part = pl.ds(x * rows, rows)
        total = 0.0
        for step in range(nh):
            block = jnp.concatenate(
                [mine_ref[step, part, :], other_ref[step, part, :]], axis=1
            )
            total = total + jnp.dot(block, weights[step], preferred_element_type=f32)
        out_ref[x] = total.astype(bf16)


def sum_kernel(in_ref, out_ref):
    total = in_ref[0].astype(f32)
    for i in range(1, in_ref.shape[0]):
        total = total + in_ref[i].astype(f32)
    out_ref[...] = total.astype(bf16).reshape(out_ref.shape)


def mix_kernel(in_ref, place_ref, gate_ref, labels_ref, seg_ref, res_ref, own_ref, out_ref, score_ref):
    ny, own_count, _ = out_ref.shape
    count, columns = labels_ref.shape
    expert = lax.axis_index("y")
    total = in_ref[0].astype(f32)
    for i in range(1, in_ref.shape[0]):
        total = total + in_ref[i].astype(f32)
    rows = total.astype(bf16)
    picked = lax.dot_general(
        place_ref[...], rows, (((0,), (0,)), ((), ())), preferred_element_type=f32
    )
    weighted = (gate_ref[:, 0:1] * picked).astype(bf16)
    row_score = jnp.sum(
        weighted.astype(f32) * labels_ref[...].astype(f32), axis=1, keepdims=True
    )
    score_ref[...] = jnp.broadcast_to(row_score, (count, LANES))
    own = jnp.sum(
        res_ref[...].astype(f32) * own_ref[...].astype(f32), axis=1, keepdims=True
    )
    at = pl.ds(pl.multiple_of(expert * own_count, own_count), own_count)
    score_ref[at, :] = score_ref[at, :] + jnp.broadcast_to(own, (own_count, LANES))
    sequence = column(seg_ref[...].astype(f32))
    lane = lax.broadcasted_iota(jnp.int32, (count, LANES), 1).astype(f32)
    member = jnp.where(sequence == lane, score_ref[...], 0.0)
    score = jnp.sum(member, axis=0, keepdims=True)
    first = score.astype(bf16).astype(f32)
    second = (score - first).astype(bf16).astype(f32)
    third = score - first - second
    row = lax.broadcasted_iota(jnp.int32, (own_count, LANES), 0)
    pads = jnp.where(
        row == 0,
        first,
        jnp.where(row == 1, second, jnp.where(row == 2, third, 0.0)),
    ).astype(bf16)
    for y in range(ny):
        out_ref[y, :, :columns] = weighted[y * own_count : (y + 1) * own_count]
        out_ref[y, :, columns:] = pads


def out_kernel(in_ref, res_ref, out_ref, score_ref):
    columns = out_ref.shape[1]
    total = in_ref[0].astype(f32)
    for y in range(1, in_ref.shape[0]):
        total = total + in_ref[y].astype(f32)
    out_ref[...] = (res_ref[...].astype(f32) + total[:, :columns]).astype(bf16)
    score = jnp.sum(total[:, columns:], axis=0, keepdims=True)
    for i in range(score_ref.shape[0]):
        score_ref[i] = score


def make_body(sizes):
    nx, nl, ny, nh, nc = sizes

    def shifted(array, dz=0, dc=0):
        return lax.ppermute(array, AXES, shift_pairs(sizes, dz, dc))

    def body(
        tokens,
        norm_gain,
        expert_ids,
        gate_weights,
        w_gate,
        w_up,
        w_down,
        label_rows,
        seg_ids,
        pair_slot,
        ref_scores,
    ):
        count, width = tokens.shape
        half = width // nc
        columns = width // (nh * nc)
        own_count = count // ny
        units = w_gate.shape[2]
        sds = jax.ShapeDtypeStruct
        own, own_far, place, gate, residual = call(
            functools.partial(front_kernel, own_count, columns),
            (
                sds((nx, SLOTS, half), bf16),
                sds((SLOTS, half), bf16),
                sds((SLOTS, count), bf16),
                sds((count, LANES), f32),
                sds((own_count, columns), bf16),
            ),
            (tokens, norm_gain[None, :], expert_ids.T, gate_weights.T),
            spare=60,
        )
        near = exchange(own, "x").reshape(nx * SLOTS, half)
        far = shifted(own_far, dz=2)
        w_send, w_mine = call(
            slice_kernel,
            (sds((2, half, units), bf16),) * 2,
            (w_gate, w_up),
            in_specs=[ANY, ANY],
            scratch=[pltpu.SemaphoreType.DMA((4,))],
            spare=60,
        )
        w_other = shifted(w_send, dc=1)
        below = shifted(near, dz=1)
        above = shifted(near, dz=-1)
        (far,) = call(far_kernel, (sds((nx, SLOTS, half), bf16),), (far,))
        far = exchange(far, "x").reshape(nx * SLOTS, half)
        early_other = dots(near, far, w_other)
        early_mine = dots(near, far, w_mine)
        below, above, early_mine = lax.optimization_barrier((below, above, early_mine))
        other = dots(below, above, w_other, early_other)
        theirs = shifted(other, dc=1)
        mine = dots(below, above, w_mine, early_mine)
        (hidden,) = call(
            hidden_kernel, (sds((nx, nl, SLOTS, units), bf16),), (mine, theirs)
        )
        hidden = hidden.reshape(nx * nl * SLOTS, units)
        labels = exchange(for_each(label_rows, ny), "y").reshape(count, columns)
        before = shifted(hidden, dz=nl)
        after = shifted(hidden, dz=-nl)
        (mine,) = call(
            stack_kernel, (sds((nh, *hidden.shape), bf16),), (hidden, after, before)
        )
        mine, labels = lax.optimization_barrier((mine, labels))
        others = shifted(mine, dc=1)
        (by_x,) = call(
            functools.partial(down_kernel, nh),
            (sds((nx, nl * SLOTS, columns), bf16),),
            (mine, others, w_down),
            flops=2 * hidden.shape[0] * w_down.shape[1] * columns,
        )
        by_x = exchange(by_x, "x")
        (by_zl,) = call(sum_kernel, (sds((nl, SLOTS, columns), bf16),), (by_x,))
        by_zl = exchange(by_zl, "zl")
        (sent,) = call(
            mix_kernel,
            (sds((ny, own_count, columns + LANES), bf16),),
            (by_zl, place, gate, labels, seg_ids, residual, label_rows),
            scratch=[pltpu.VMEM((count, LANES), f32)],
        )
        terms = exchange(sent, "y")
        layer_out, partial_value = call(
            out_kernel,
            (sds((own_count, columns), bf16), sds((nh * nc, 1, LANES), f32)),
            (terms, residual),
        )
        totals = exchange(partial_value, TENSOR)
        totals = jnp.sum(totals, axis=(0, 1))[:SEQS]
        slots_here = pair_slot[0]
        polarity = (1 - 2 * (slots_here % 2)).astype(f32)
        pair_member = (
            (slots_here // 2)[:, None]
            == jnp.arange(PAIRS, dtype=jnp.int32)[None, :]
        ).astype(f32)
        margins = dpo_beta * jnp.sum(
            pair_member * (polarity * (totals - ref_scores[0]))[:, None], axis=0
        )
        return (layer_out, margins[None, :])

    return body


def solution(mesh):
    sizes = (4, 4, mesh.shape["expert"], 3, 2)
    fine = Mesh(mesh.devices.reshape(sizes), AXES)
    placed = (
        P(DP, None),
        P(),
        P(DP, None),
        P(DP, None),
        P("y", None, (*DP, *TENSOR)),
        P("y", None, (*DP, *TENSOR)),
        P("y", DP, TENSOR),
        P((*DP, "y"), TENSOR),
        P(DP, None),
        P(DP, None),
        P(DP, None),
    )
    return jax.shard_map(
        make_body(sizes),
        mesh=fine,
        in_specs=placed,
        out_specs=(P((*DP, "y"), TENSOR), P(DP, None)),
        check_vma=False,
    )
```

```python
import functools

import jax
import jax.numpy as jnp
from jax import lax
from jax.experimental import pallas as pl
from jax.experimental.pallas import tpu as pltpu
from jax.sharding import Mesh, PartitionSpec as P

SEQS = 4
PAIRS = 2
SLOTS = 36
LANES = 128
epsilon = 1e-05
dpo_beta = 0.5

AXES = ("x", "zl", "y", "zh", "c")
DP = ("x", "zl")
TENSOR = ("zh", "c")
OFFSETS = (0, 2, -1, 1)


f32 = jnp.float32
bf16 = jnp.bfloat16
VMEM = pl.BlockSpec(memory_space=pltpu.VMEM)
HBM = pl.BlockSpec(memory_space=pltpu.HBM)


def shift_pairs(sizes, dx=0, dy=0, dz=0, dc=0):
    nx, nl, ny, nh, nc = sizes
    nz = nh * nl

    def flat(x, y, z, c):
        return (((x * nl + z % nl) * ny + y) * nh + z // nl) * nc + c

    return [
        (
            flat(x, y, z, c),
            flat((x + dx) % nx, (y + dy) % ny, (z + dz) % nz, (c + dc) % nc),
        )
        for x in range(nx)
        for y in range(ny)
        for z in range(nz)
        for c in range(nc)
    ]


def exchange(array, axis):
    return lax.all_to_all(array, axis, 0, 0, tiled=True)


def call(kernel, outs, ins, flops=0, in_specs=None, scratch=(), spare=4):
    size = sum(a.size * a.dtype.itemsize for a in (*ins, *outs))
    limit = min(size + (spare << 20), 60 << 20)
    return pl.pallas_call(
        kernel,
        out_shape=outs,
        in_specs=in_specs or [VMEM] * len(ins),
        out_specs=tuple(VMEM for _ in outs),
        scratch_shapes=list(scratch),
        compiler_params=pltpu.CompilerParams(vmem_limit_bytes=limit),
        cost_estimate=pl.CostEstimate(
            flops=flops or size, bytes_accessed=size, transcendentals=0
        ),
    )(*ins)


def column(row):
    return jnp.transpose(jnp.broadcast_to(row, (LANES, LANES)))


def front_kernel(own_count, columns, *refs):
    *ins, own_ref, far_ref, place_ref, gate_ref, res_ref, tok_ref, gain_ref, ids_ref, gw_ref, sems = refs
    copies = [
        pltpu.make_async_copy(ref, held, sems.at[i])
        for i, (ref, held) in enumerate(
            zip(ins, (tok_ref, gain_ref, ids_ref, gw_ref), strict=True)
        )
    ]
    for copy in copies:
        copy.start()
    for copy in copies:
        copy.wait()
    count, width = tok_ref.shape
    expert = lax.axis_index("y")
    core = lax.axis_index("c")
    step = 512
    squares = jnp.zeros((count, step), f32)
    for start in range(0, width, step):
        v = tok_ref[:, start : start + step].astype(f32)
        squares = squares + v * v
    total = jnp.sum(squares, axis=1, keepdims=True)
    inverse_rms = lax.rsqrt(total * (1.0 / width) + epsilon)
    match = ids_ref[...] == expert
    hit = match.astype(f32)
    named = hit[0:1] + hit[1:2]
    gate_row = jnp.sum(jnp.where(match, gw_ref[...], 0.0), axis=0, keepdims=True)
    gate_ref[...] = column(gate_row)
    before = lax.broadcasted_iota(jnp.int32, (count, count), 0)
    after = lax.broadcasted_iota(jnp.int32, (count, count), 1)
    position = jnp.dot(
        jnp.broadcast_to(named, (8, count)).astype(bf16),
        (before < after).astype(bf16),
        preferred_element_type=f32,
    )[0:1]
    slot = lax.broadcasted_iota(jnp.int32, (2 * SLOTS, count), 0).astype(f32)
    here = named > 0.5
    upper = jnp.where((slot == position) & here, 1.0, 0.0).astype(bf16)
    lower = jnp.where((slot - SLOTS == position) & here, 1.0, 0.0).astype(bf16)
    place_ref[...] = upper
    fold = own_ref.shape[2]
    half = 2 * fold
    nc = width // half
    column_at = (lax.axis_index("zh") * nc + core) * columns
    res_ref[...] = tok_ref[
        pl.ds(pl.multiple_of(expert * own_count, own_count), own_count),
        pl.ds(pl.multiple_of(column_at, LANES), columns),
    ]

    def normed(start):
        at = pl.multiple_of(core * half + start, LANES)
        v = tok_ref[:, pl.ds(at, step)].astype(f32)
        return (v * inverse_rms * gain_ref[:, pl.ds(at, step)]).astype(bf16)

    for start in range(0, fold, step):
        rows = jnp.dot(upper, normed(start), preferred_element_type=f32)
        rows += jnp.dot(lower, normed(start + fold), preferred_element_type=f32)
        rows = rows.astype(bf16)
        for x in range(own_ref.shape[0]):
            own_ref[x, :, start : start + step] = rows
        far_ref[:, start : start + step] = rows


def copies_kernel(in_ref, out_ref):
    for x in range(out_ref.shape[0]):
        out_ref[x] = in_ref[...]


def pack_kernel(in_ref, out_ref):
    blocks, folded, fold = in_ref.shape
    rows = out_ref.shape[0]
    step = 512
    to = lax.broadcasted_iota(jnp.int32, (rows, blocks * folded), 0)
    source = lax.broadcasted_iota(jnp.int32, (rows, blocks * folded), 1)
    for side in range(2):
        at = jnp.where(source < 0, 0, -1)
        for x in range(blocks):
            base = x * folded + side * SLOTS
            inside = (source >= base) & (source < base + SLOTS)
            at = jnp.where(inside, source - base + x * SLOTS, at)
        chosen = jnp.where(at == to, 1.0, 0.0).astype(bf16)
        for start in range(0, fold, step):
            block = jnp.concatenate(
                [in_ref[x, :, start : start + step] for x in range(blocks)], axis=0
            )
            moved = jnp.dot(chosen, block, preferred_element_type=f32).astype(bf16)
            out_ref[:, side * fold + start : side * fold + start + step] = moved


def slice_kernel(gate_ref, up_ref, send_ref, keep_ref, sems):
    half = send_ref.shape[1]
    core = lax.axis_index("c")
    copies = []
    for i, ref in enumerate((gate_ref, up_ref)):
        for j, (out, c) in enumerate(((send_ref, 1 - core), (keep_ref, core))):
            at = pl.multiple_of(c * half, 8)
            copies.append(
                pltpu.make_async_copy(
                    ref.at[0, pl.ds(at, half)], out.at[i], sems.at[2 * i + j]
                )
            )
    for copy in copies:
        copy.start()
    for copy in copies:
        copy.wait()


def dots_kernel(a_ref, b_ref, w_ref, *refs):
    *first, out_ref, sum_ref = refs
    _, half = a_ref.shape
    step = 512
    sum_ref[...] = jnp.zeros_like(sum_ref)

    def body(k, _):
        at = pl.multiple_of(k * step, step)
        x = jnp.concatenate(
            [a_ref[:, pl.ds(at, step)], b_ref[:, pl.ds(at, step)]], axis=0
        )
        w = jnp.concatenate(
            [w_ref[0, pl.ds(at, step), :], w_ref[1, pl.ds(at, step), :]], axis=1
        )
        sum_ref[...] += jnp.dot(x, w, preferred_element_type=f32)
        return 0

    lax.fori_loop(0, half // step, body, 0)
    at = 0
    for ref in first:
        out_ref[at : at + ref.shape[0]] = ref[...]
        at += ref.shape[0]
    out_ref[at:] = sum_ref[...]


def dots(a, b, w, *first):
    rows, half = a.shape
    wide = 2 * w.shape[2]
    out = jax.ShapeDtypeStruct((2 * rows + sum(p.shape[0] for p in first), wide), f32)
    (sums,) = call(
        dots_kernel,
        (out,),
        (a, b, w, *first),
        flops=2 * 2 * rows * half * wide,
        scratch=[pltpu.VMEM((2 * rows, wide), f32)],
    )
    return sums


def hidden_kernel(nx, mine_ref, theirs_ref, out_ref):
    _, total, units = out_ref.shape
    block = total // nx
    parts = []
    for start in range(0, total, block):
        sums = mine_ref[start : start + block] + theirs_ref[start : start + block]
        gate, up = sums[:, :units], sums[:, units:]
        parts.append((gate / (1.0 + jnp.exp(-gate)) * up).astype(bf16))
    hidden = jnp.concatenate(parts, axis=0)
    slot = lax.broadcasted_iota(jnp.int32, (block, total), 0)
    source = lax.broadcasted_iota(jnp.int32, (block, total), 1)
    for x in range(nx):
        at = jnp.where(source < 0, 0, -1)
        for r in range(total // block):
            base = r * block + x * SLOTS
            inside = (source >= base) & (source < base + SLOTS)
            at = jnp.where(inside, source - base + r * SLOTS, at)
        chosen = jnp.where(at == slot, 1.0, 0.0).astype(bf16)
        moved = jnp.dot(chosen, hidden, preferred_element_type=f32)
        moved = moved.astype(bf16)
        for i in range(out_ref.shape[0]):
            out_ref[i, x * block : (x + 1) * block] = moved


def down_kernel(mine_ref, other_ref, w_ref, out_ref):
    nx, rows, _ = out_ref.shape
    nh, _, units = mine_ref.shape
    core = lax.axis_index("c")
    weights = []
    for step in range(nh):
        base = step * 2
        weights.append(
            jnp.concatenate(
                [
                    w_ref[0, pl.ds(pl.multiple_of((base + c) * units, units), units), :]
                    for c in (core, 1 - core)
                ],
                axis=0,
            )
        )
    for x in range(nx):
        part = pl.ds(x * rows, rows)
        total = 0.0
        for step in range(nh):
            block = jnp.concatenate(
                [mine_ref[step, part, :], other_ref[step, part, :]], axis=1
            )
            total = total + jnp.dot(block, weights[step], preferred_element_type=f32)
        out_ref[x] = total.astype(bf16)


def sum_kernel(in_ref, out_ref):
    nl, slots, _ = out_ref.shape
    rows = in_ref.shape[1]
    zl = lax.axis_index("zl")
    total = in_ref[0].astype(f32)
    for i in range(1, in_ref.shape[0]):
        total = total + in_ref[i].astype(f32)
    total = total.astype(bf16)
    slot = lax.broadcasted_iota(jnp.int32, (slots, rows), 0)
    source = lax.broadcasted_iota(jnp.int32, (slots, rows), 1)
    for r, offset in enumerate(OFFSETS):
        chosen = jnp.where(source == slot + r * SLOTS, 1.0, 0.0).astype(bf16)
        moved = jnp.dot(chosen, total, preferred_element_type=f32)
        out_ref[lax.rem(zl + offset + nl, nl)] = moved.astype(bf16)


def join_kernel(a_ref, b_ref, out_ref):
    size = a_ref.shape[0]
    out_ref[:size] = a_ref[...]
    out_ref[size:] = b_ref[...]


def mix_kernel(in_ref, place_ref, gate_ref, labels_ref, seg_ref, res_ref, own_ref, out_ref, score_ref):
    ny, own_count, _ = out_ref.shape
    count, columns = ny * own_count, labels_ref.shape[2]
    expert = lax.axis_index("y")
    total = in_ref[0].astype(f32)
    for i in range(1, in_ref.shape[0]):
        total = total + in_ref[i].astype(f32)
    rows = jnp.concatenate(
        [
            total.astype(bf16),
            jnp.zeros((place_ref.shape[0] - total.shape[0], columns), bf16),
        ],
        axis=0,
    )
    picked = lax.dot_general(
        place_ref[...], rows, (((0,), (0,)), ((), ())), preferred_element_type=f32
    )
    weighted = (gate_ref[:, 0:1] * picked).astype(bf16)
    for y in range(ny):
        rows = slice(y * own_count, (y + 1) * own_count)
        label = labels_ref[lax.rem(expert - y + ny, ny)].astype(f32)
        row_score = jnp.sum(
            weighted[rows].astype(f32) * label, axis=1, keepdims=True
        )
        score_ref[rows, :] = jnp.broadcast_to(row_score, (own_count, LANES))
    own = jnp.sum(
        res_ref[...].astype(f32) * own_ref[...].astype(f32), axis=1, keepdims=True
    )
    at = pl.ds(pl.multiple_of(expert * own_count, own_count), own_count)
    score_ref[at, :] = score_ref[at, :] + jnp.broadcast_to(own, (own_count, LANES))
    sequence = column(seg_ref[...].astype(f32))
    lane = lax.broadcasted_iota(jnp.int32, (count, LANES), 1).astype(f32)
    member = jnp.where(sequence == lane, score_ref[...], 0.0)
    score = jnp.sum(member, axis=0, keepdims=True)
    first = score.astype(bf16).astype(f32)
    second = (score - first).astype(bf16).astype(f32)
    third = score - first - second
    row = lax.broadcasted_iota(jnp.int32, (own_count, LANES), 0)
    pads = jnp.where(
        row == 0,
        first,
        jnp.where(row == 1, second, jnp.where(row == 2, third, 0.0)),
    ).astype(bf16)
    for y in range(ny):
        out_ref[y, :, :columns] = weighted[y * own_count : (y + 1) * own_count]
        out_ref[y, :, columns:] = pads


def score_kernel(columns, in_ref, score_ref):
    total = in_ref[0, :, columns:].astype(f32)
    for y in range(1, in_ref.shape[0]):
        total = total + in_ref[y, :, columns:].astype(f32)
    score = jnp.sum(total, axis=0, keepdims=True)
    for i in range(score_ref.shape[0]):
        score_ref[i] = score


def out_kernel(in_ref, res_ref, out_ref):
    columns = out_ref.shape[1]
    total = in_ref[0, :, :columns].astype(f32)
    for y in range(1, in_ref.shape[0]):
        total = total + in_ref[y, :, :columns].astype(f32)
    out_ref[...] = (res_ref[...].astype(f32) + total).astype(bf16)


def margin_kernel(in_ref, slot_ref, ref_ref, out_ref):
    total = in_ref[0]
    for i in range(1, in_ref.shape[0]):
        total = total + in_ref[i]
    slots = slot_ref[...]
    pair = lax.shift_right_logical(slots, 1)
    polarity = (1 - 2 * (slots - 2 * pair)).astype(f32)
    signed = polarity * (total[:, :SEQS] - ref_ref[...])
    sums = [
        jnp.sum(jnp.where(pair == p, signed, 0.0), axis=1, keepdims=True)
        for p in range(PAIRS)
    ]
    out_ref[...] = dpo_beta * jnp.concatenate(sums, axis=1)


def make_body(sizes):
    nx, nl, ny, nh, nc = sizes

    def shifted(array, **shift):
        return lax.ppermute(array, AXES, shift_pairs(sizes, **shift))

    def body(
        tokens,
        norm_gain,
        expert_ids,
        gate_weights,
        w_gate,
        w_up,
        w_down,
        label_rows,
        seg_ids,
        pair_slot,
        ref_scores,
    ):
        count, width = tokens.shape
        half = width // nc
        fold = half // 2
        columns = width // (nh * nc)
        own_count = count // ny
        units = w_gate.shape[2]
        sds = jax.ShapeDtypeStruct
        own, own_far, place, gate, residual = call(
            functools.partial(front_kernel, own_count, columns),
            (
                sds((nx, 2 * SLOTS, fold), bf16),
                sds((2 * SLOTS, fold), bf16),
                sds((2 * SLOTS, count), bf16),
                sds((count, LANES), f32),
                sds((own_count, columns), bf16),
            ),
            (tokens, norm_gain[None, :], expert_ids.T, gate_weights.T),
            in_specs=[HBM] * 4,
            scratch=[
                pltpu.VMEM((count, width), bf16),
                pltpu.VMEM((1, width), f32),
                pltpu.VMEM((2, count), jnp.int32),
                pltpu.VMEM((2, count), f32),
                pltpu.SemaphoreType.DMA((4,)),
            ],
            spare=60,
        )
        near = exchange(own, "x")
        far = shifted(own_far, dz=2)
        w_send, w_mine = call(
            slice_kernel,
            (sds((2, half, units), bf16),) * 2,
            (w_gate, w_up),
            in_specs=[HBM, HBM],
            scratch=[pltpu.SemaphoreType.DMA((4,))],
            spare=60,
        )
        w_other = shifted(w_send, dc=1)
        (near,) = call(pack_kernel, (sds((nx * SLOTS, half), bf16),), (near,))
        below = shifted(near, dz=1)
        above = shifted(near, dz=-1)
        (far,) = call(copies_kernel, (sds(own.shape, bf16),), (far,))
        far = exchange(far, "x")
        (far,) = call(pack_kernel, (sds((nx * SLOTS, half), bf16),), (far,))
        early_other = dots(near, far, w_other)
        early_mine = dots(near, far, w_mine)
        below, above, early_mine = lax.optimization_barrier((below, above, early_mine))
        other = dots(below, above, w_other, early_other)
        theirs = shifted(other, dc=1)
        mine = dots(below, above, w_mine, early_mine)
        (hidden,) = call(
            functools.partial(hidden_kernel, nx),
            (sds((nh, nx * nl * SLOTS, units), bf16),),
            (mine, theirs),
        )
        mine = exchange(hidden, "zh")
        labels = label_rows[None]
        while labels.shape[0] < ny:
            size = labels.shape[0]
            arrived = shifted(labels, dy=size)
            (labels,) = call(
                join_kernel,
                (sds((2 * size, own_count, columns), bf16),),
                (labels, arrived),
            )
        others = shifted(mine, dc=1)
        (by_x,) = call(
            down_kernel,
            (sds((nx, nl * SLOTS, columns), bf16),),
            (mine, others, w_down),
            flops=2 * hidden.shape[1] * w_down.shape[1] * columns,
        )
        by_x = exchange(by_x, "x")
        (by_zl,) = call(sum_kernel, (sds((nl, SLOTS, columns), bf16),), (by_x,))
        by_zl, labels = lax.optimization_barrier((by_zl, labels))
        by_zl = exchange(by_zl, "zl")
        (sent,) = call(
            mix_kernel,
            (sds((ny, own_count, columns + LANES), bf16),),
            (by_zl, place, gate, labels, seg_ids, residual, label_rows),
            scratch=[pltpu.VMEM((count, LANES), f32)],
        )
        terms = exchange(sent, "y")
        (score,) = call(
            functools.partial(score_kernel, columns),
            (sds((nh * nc, 1, LANES), f32),),
            (terms,),
        )
        scores = exchange(score, TENSOR)
        (layer_out,) = call(
            out_kernel, (sds((own_count, columns), bf16),), (terms, residual)
        )
        (margins,) = call(
            margin_kernel, (sds((1, PAIRS), f32),), (scores, pair_slot, ref_scores)
        )
        return (layer_out, margins)

    return body


def solution(mesh):
    sizes = (4, 4, mesh.shape["expert"], 3, 2)
    fine = Mesh(mesh.devices.reshape(sizes), AXES)
    placed = (
        P(DP, None),
        P(),
        P(DP, None),
        P(DP, None),
        P("y", None, (*DP, *TENSOR)),
        P("y", None, (*DP, *TENSOR)),
        P("y", DP, TENSOR),
        P((*DP, "y"), TENSOR),
        P(DP, None),
        P(DP, None),
        P(DP, None),
    )
    return jax.shard_map(
        make_body(sizes),
        mesh=fine,
        in_specs=placed,
        out_specs=(P((*DP, "y"), TENSOR), P(DP, None)),
        check_vma=False,
    )
```

```python
import functools

import jax
import jax.numpy as jnp
from jax import lax
from jax.experimental import pallas as pl
from jax.experimental.pallas import tpu as pltpu
from jax.sharding import Mesh, PartitionSpec as P

SEQS = 4
PAIRS = 2
SLOTS = 36
LANES = 128
epsilon = 1e-05
dpo_beta = 0.5

AXES = ("x", "zl", "y", "zh", "c")
DP = ("x", "zl")
TENSOR = ("zh", "c")
OFFSETS = (0, 2, -1, 1)


f32 = jnp.float32
bf16 = jnp.bfloat16
VMEM = pl.BlockSpec(memory_space=pltpu.VMEM)
HBM = pl.BlockSpec(memory_space=pltpu.HBM)


def shift_pairs(sizes, dx=0, dy=0, dz=0, dc=0, cross=1):
    nx, nl, ny, nh, nc = sizes
    nz = nh * nl

    def flat(x, y, z, c):
        return (((x * nl + z % nl) * ny + y) * nh + z // nl) * nc + c

    pairs = []
    for x in range(nx):
        for y in range(ny):
            for z in range(nz):
                for c in range(nc):
                    way = cross if c else 1
                    target = flat(
                        (x + way * dx) % nx,
                        (y + dy) % ny,
                        (z + way * dz) % nz,
                        (c + dc) % nc,
                    )
                    pairs.append((flat(x, y, z, c), target))
    return pairs


def exchange(array, axis):
    return lax.all_to_all(array, axis, 0, 0, tiled=True)


def call(kernel, outs, ins, flops=0, in_specs=None, scratch=(), spare=4):
    size = sum(a.size * a.dtype.itemsize for a in (*ins, *outs))
    limit = min(size + (spare << 20), 60 << 20)
    return pl.pallas_call(
        kernel,
        out_shape=outs,
        in_specs=in_specs or [VMEM] * len(ins),
        out_specs=tuple(VMEM for _ in outs),
        scratch_shapes=list(scratch),
        compiler_params=pltpu.CompilerParams(vmem_limit_bytes=limit),
        cost_estimate=pl.CostEstimate(
            flops=flops or size, bytes_accessed=size, transcendentals=0
        ),
    )(*ins)


def column(row):
    return jnp.transpose(jnp.broadcast_to(row, (LANES, LANES)))


def front_kernel(own_count, columns, *refs):
    *ins, own_ref, far_ref, place_ref, gate_ref, res_ref, tok_ref, gain_ref, ids_ref, gw_ref, sems = refs
    copies = [
        pltpu.make_async_copy(ref, held, sems.at[i])
        for i, (ref, held) in enumerate(
            zip(ins, (tok_ref, gain_ref, ids_ref, gw_ref), strict=True)
        )
    ]
    for copy in copies:
        copy.start()
    for copy in copies:
        copy.wait()
    count, width = tok_ref.shape
    expert = lax.axis_index("y")
    core = lax.axis_index("c")
    step = 512
    squares = jnp.zeros((count, step), f32)
    for start in range(0, width, step):
        v = tok_ref[:, start : start + step].astype(f32)
        squares = squares + v * v
    total = jnp.sum(squares, axis=1, keepdims=True)
    inverse_rms = lax.rsqrt(total * (1.0 / width) + epsilon)
    match = ids_ref[...] == expert
    hit = match.astype(f32)
    named = hit[0:1] + hit[1:2]
    gate_row = jnp.sum(jnp.where(match, gw_ref[...], 0.0), axis=0, keepdims=True)
    gate_ref[...] = column(gate_row)
    before = lax.broadcasted_iota(jnp.int32, (count, count), 0)
    after = lax.broadcasted_iota(jnp.int32, (count, count), 1)
    position = jnp.dot(
        jnp.broadcast_to(named, (8, count)).astype(bf16),
        (before < after).astype(bf16),
        preferred_element_type=f32,
    )[0:1]
    slot = lax.broadcasted_iota(jnp.int32, (2 * SLOTS, count), 0).astype(f32)
    here = named > 0.5
    upper = jnp.where((slot == position) & here, 1.0, 0.0).astype(bf16)
    lower = jnp.where((slot - SLOTS == position) & here, 1.0, 0.0).astype(bf16)
    place_ref[...] = upper
    fold = own_ref.shape[2]
    half = 2 * fold
    nc = width // half
    column_at = (lax.axis_index("zh") * nc + core) * columns
    res_ref[...] = tok_ref[
        pl.ds(pl.multiple_of(expert * own_count, own_count), own_count),
        pl.ds(pl.multiple_of(column_at, LANES), columns),
    ]

    def normed(start):
        at = pl.multiple_of(core * half + start, LANES)
        v = tok_ref[:, pl.ds(at, step)].astype(f32)
        return (v * inverse_rms * gain_ref[:, pl.ds(at, step)]).astype(bf16)

    for start in range(0, fold, step):
        rows = jnp.dot(upper, normed(start), preferred_element_type=f32)
        rows += jnp.dot(lower, normed(start + fold), preferred_element_type=f32)
        rows = rows.astype(bf16)
        for x in range(own_ref.shape[0]):
            own_ref[x, :, start : start + step] = rows
        far_ref[:, start : start + step] = rows


def copies_kernel(in_ref, out_ref):
    for x in range(out_ref.shape[0]):
        out_ref[x] = in_ref[...]


def pack_kernel(in_ref, out_ref):
    blocks, folded, fold = in_ref.shape
    rows = out_ref.shape[0]
    step = 512
    to = lax.broadcasted_iota(jnp.int32, (rows, blocks * folded), 0)
    source = lax.broadcasted_iota(jnp.int32, (rows, blocks * folded), 1)
    for side in range(2):
        at = jnp.where(source < 0, 0, -1)
        for x in range(blocks):
            base = x * folded + side * SLOTS
            inside = (source >= base) & (source < base + SLOTS)
            at = jnp.where(inside, source - base + x * SLOTS, at)
        chosen = jnp.where(at == to, 1.0, 0.0).astype(bf16)
        for start in range(0, fold, step):
            block = jnp.concatenate(
                [in_ref[x, :, start : start + step] for x in range(blocks)], axis=0
            )
            moved = jnp.dot(chosen, block, preferred_element_type=f32).astype(bf16)
            out_ref[:, side * fold + start : side * fold + start + step] = moved


def slice_kernel(gate_ref, up_ref, send_ref, keep_ref, sems):
    half = send_ref.shape[1]
    core = lax.axis_index("c")
    copies = []
    for i, ref in enumerate((gate_ref, up_ref)):
        for j, (out, c) in enumerate(((send_ref, 1 - core), (keep_ref, core))):
            at = pl.multiple_of(c * half, 8)
            copies.append(
                pltpu.make_async_copy(
                    ref.at[0, pl.ds(at, half)], out.at[i], sems.at[2 * i + j]
                )
            )
    for copy in copies:
        copy.start()
    for copy in copies:
        copy.wait()


def dots_kernel(a_ref, b_ref, w_ref, *refs):
    *first, out_ref, sum_ref = refs
    rows, half = a_ref.shape
    step = 512
    sum_ref[...] = jnp.zeros_like(sum_ref)

    def body(k, _):
        at = pl.multiple_of(k * step, step)
        x = jnp.concatenate(
            [a_ref[:, pl.ds(at, step)], b_ref[:, pl.ds(at, step)]], axis=0
        )
        w = jnp.concatenate(
            [w_ref[0, pl.ds(at, step), :], w_ref[1, pl.ds(at, step), :]], axis=1
        )
        sum_ref[...] += jnp.dot(x, w, preferred_element_type=f32)
        return 0

    lax.fori_loop(0, half // step, body, 0)
    at = 0
    for ref in first:
        out_ref[at : at + ref.shape[0]] = ref[...]
        at += ref.shape[0]
    if not first:
        out_ref[...] = sum_ref[...]
        return
    core = lax.axis_index("c")
    for i in range(2):
        to = pl.multiple_of(at + lax.rem(core + i, 2) * rows, 16)
        out_ref[pl.ds(to, rows), :] = sum_ref[i * rows : (i + 1) * rows]


def dots(a, b, w, *first):
    rows, half = a.shape
    wide = 2 * w.shape[2]
    out = jax.ShapeDtypeStruct((2 * rows + sum(p.shape[0] for p in first), wide), f32)
    (sums,) = call(
        dots_kernel,
        (out,),
        (a, b, w, *first),
        flops=2 * 2 * rows * half * wide,
        scratch=[pltpu.VMEM((2 * rows, wide), f32)],
    )
    return sums


def hidden_kernel(nx, mine_ref, theirs_ref, out_ref):
    total, units = out_ref.shape
    block = total // nx
    parts = []
    for start in range(0, total, block):
        sums = mine_ref[start : start + block] + theirs_ref[start : start + block]
        gate, up = sums[:, :units], sums[:, units:]
        parts.append((gate / (1.0 + jnp.exp(-gate)) * up).astype(bf16))
    hidden = jnp.concatenate(parts, axis=0)
    slot = lax.broadcasted_iota(jnp.int32, (block, total), 0)
    source = lax.broadcasted_iota(jnp.int32, (block, total), 1)
    for x in range(nx):
        at = jnp.where(source < 0, 0, -1)
        for r in range(total // block):
            base = r * block + x * SLOTS
            inside = (source >= base) & (source < base + SLOTS)
            at = jnp.where(inside, source - base + r * SLOTS, at)
        chosen = jnp.where(at == slot, 1.0, 0.0).astype(bf16)
        moved = jnp.dot(chosen, hidden, preferred_element_type=f32)
        out_ref[x * block : (x + 1) * block] = moved.astype(bf16)


def stack_kernel(own_ref, first_ref, second_ref, out_ref):
    core = lax.axis_index("c")
    out_ref[0] = own_ref[...]
    out_ref[2 - core] = first_ref[...]
    out_ref[1 + core] = second_ref[...]


def down_kernel(nh, mine_ref, other_ref, w_ref, out_ref):
    nx, rows, _ = out_ref.shape
    units = mine_ref.shape[2]
    zh = lax.axis_index("zh")
    core = lax.axis_index("c")
    weights = []
    for step in range(nh):
        base = lax.rem(zh + step, nh) * 2
        weights.append(
            jnp.concatenate(
                [
                    w_ref[0, pl.ds(pl.multiple_of((base + c) * units, units), units), :]
                    for c in (core, 1 - core)
                ],
                axis=0,
            )
        )
    for x in range(nx):
        part = pl.ds(x * rows, rows)
        total = 0.0
        for step in range(nh):
            block = jnp.concatenate(
                [mine_ref[step, part, :], other_ref[step, part, :]], axis=1
            )
            total = total + jnp.dot(block, weights[step], preferred_element_type=f32)
        out_ref[x] = total.astype(bf16)


def sum_kernel(in_ref, out_ref):
    nl, slots, _ = out_ref.shape
    rows = in_ref.shape[1]
    zl = lax.axis_index("zl")
    total = in_ref[0].astype(f32)
    for i in range(1, in_ref.shape[0]):
        total = total + in_ref[i].astype(f32)
    total = total.astype(bf16)
    slot = lax.broadcasted_iota(jnp.int32, (slots, rows), 0)
    source = lax.broadcasted_iota(jnp.int32, (slots, rows), 1)
    for r, offset in enumerate(OFFSETS):
        chosen = jnp.where(source == slot + r * SLOTS, 1.0, 0.0).astype(bf16)
        moved = jnp.dot(chosen, total, preferred_element_type=f32)
        out_ref[lax.rem(zl + offset + nl, nl)] = moved.astype(bf16)


def join_kernel(a_ref, b_ref, out_ref):
    size = a_ref.shape[0]
    out_ref[:size] = a_ref[...]
    out_ref[size:] = b_ref[...]


def mix_kernel(in_ref, place_ref, gate_ref, labels_ref, seg_ref, res_ref, own_ref, out_ref, score_ref):
    ny, own_count, _ = out_ref.shape
    count, columns = ny * own_count, labels_ref.shape[2]
    expert = lax.axis_index("y")
    total = in_ref[0].astype(f32)
    for i in range(1, in_ref.shape[0]):
        total = total + in_ref[i].astype(f32)
    rows = jnp.concatenate(
        [
            total.astype(bf16),
            jnp.zeros((place_ref.shape[0] - total.shape[0], columns), bf16),
        ],
        axis=0,
    )
    picked = lax.dot_general(
        place_ref[...], rows, (((0,), (0,)), ((), ())), preferred_element_type=f32
    )
    weighted = (gate_ref[:, 0:1] * picked).astype(bf16)
    for y in range(ny):
        rows = slice(y * own_count, (y + 1) * own_count)
        label = labels_ref[lax.rem(expert - y + ny, ny)].astype(f32)
        row_score = jnp.sum(
            weighted[rows].astype(f32) * label, axis=1, keepdims=True
        )
        score_ref[rows, :] = jnp.broadcast_to(row_score, (own_count, LANES))
    own = jnp.sum(
        res_ref[...].astype(f32) * own_ref[...].astype(f32), axis=1, keepdims=True
    )
    at = pl.ds(pl.multiple_of(expert * own_count, own_count), own_count)
    score_ref[at, :] = score_ref[at, :] + jnp.broadcast_to(own, (own_count, LANES))
    sequence = column(seg_ref[...].astype(f32))
    lane = lax.broadcasted_iota(jnp.int32, (count, LANES), 1).astype(f32)
    member = jnp.where(sequence == lane, score_ref[...], 0.0)
    score = jnp.sum(member, axis=0, keepdims=True)
    first = score.astype(bf16).astype(f32)
    second = (score - first).astype(bf16).astype(f32)
    third = score - first - second
    row = lax.broadcasted_iota(jnp.int32, (own_count, LANES), 0)
    pads = jnp.where(
        row == 0,
        first,
        jnp.where(row == 1, second, jnp.where(row == 2, third, 0.0)),
    ).astype(bf16)
    for y in range(ny):
        out_ref[y, :, :columns] = weighted[y * own_count : (y + 1) * own_count]
        out_ref[y, :, columns:] = pads


def score_kernel(columns, in_ref, score_ref):
    total = in_ref[0, :, columns:].astype(f32)
    for y in range(1, in_ref.shape[0]):
        total = total + in_ref[y, :, columns:].astype(f32)
    score = jnp.sum(total, axis=0, keepdims=True)
    for i in range(score_ref.shape[0]):
        score_ref[i] = score


def out_kernel(in_ref, res_ref, out_ref):
    columns = out_ref.shape[1]
    total = in_ref[0, :, :columns].astype(f32)
    for y in range(1, in_ref.shape[0]):
        total = total + in_ref[y, :, :columns].astype(f32)
    out_ref[...] = (res_ref[...].astype(f32) + total).astype(bf16)


def margin_kernel(in_ref, slot_ref, ref_ref, out_ref):
    total = in_ref[0]
    for i in range(1, in_ref.shape[0]):
        total = total + in_ref[i]
    slots = slot_ref[...]
    pair = lax.shift_right_logical(slots, 1)
    polarity = (1 - 2 * (slots - 2 * pair)).astype(f32)
    signed = polarity * (total[:, :SEQS] - ref_ref[...])
    sums = [
        jnp.sum(jnp.where(pair == p, signed, 0.0), axis=1, keepdims=True)
        for p in range(PAIRS)
    ]
    out_ref[...] = dpo_beta * jnp.concatenate(sums, axis=1)


def make_body(sizes):
    nx, nl, ny, nh, nc = sizes

    def shifted(array, **shift):
        return lax.ppermute(array, AXES, shift_pairs(sizes, **shift))

    def body(
        tokens,
        norm_gain,
        expert_ids,
        gate_weights,
        w_gate,
        w_up,
        w_down,
        label_rows,
        seg_ids,
        pair_slot,
        ref_scores,
    ):
        count, width = tokens.shape
        half = width // nc
        fold = half // 2
        columns = width // (nh * nc)
        own_count = count // ny
        units = w_gate.shape[2]
        sds = jax.ShapeDtypeStruct
        own, own_far, place, gate, residual = call(
            functools.partial(front_kernel, own_count, columns),
            (
                sds((nx, 2 * SLOTS, fold), bf16),
                sds((2 * SLOTS, fold), bf16),
                sds((2 * SLOTS, count), bf16),
                sds((count, LANES), f32),
                sds((own_count, columns), bf16),
            ),
            (tokens, norm_gain[None, :], expert_ids.T, gate_weights.T),
            in_specs=[HBM] * 4,
            scratch=[
                pltpu.VMEM((count, width), bf16),
                pltpu.VMEM((1, width), f32),
                pltpu.VMEM((2, count), jnp.int32),
                pltpu.VMEM((2, count), f32),
                pltpu.SemaphoreType.DMA((4,)),
            ],
            spare=60,
        )
        near = exchange(own, "x")
        far = shifted(own_far, dz=2)
        w_send, w_mine = call(
            slice_kernel,
            (sds((2, half, units), bf16),) * 2,
            (w_gate, w_up),
            in_specs=[HBM, HBM],
            scratch=[pltpu.SemaphoreType.DMA((4,))],
            spare=60,
        )
        w_other = shifted(w_send, dc=1)
        (near,) = call(pack_kernel, (sds((nx * SLOTS, half), bf16),), (near,))
        first = shifted(near, dz=1, cross=-1)
        second = shifted(near, dz=-1, cross=-1)
        (far,) = call(copies_kernel, (sds(own.shape, bf16),), (far,))
        far = exchange(far, "x")
        (far,) = call(pack_kernel, (sds((nx * SLOTS, half), bf16),), (far,))
        early_other = dots(near, far, w_other)
        early_mine = dots(near, far, w_mine)
        first, second, early_mine = lax.optimization_barrier(
            (first, second, early_mine)
        )
        other = dots(first, second, w_other, early_other)
        theirs = shifted(other, dc=1)
        mine = dots(first, second, w_mine, early_mine)
        (hidden,) = call(
            functools.partial(hidden_kernel, nx),
            (sds((nx * nl * SLOTS, units), bf16),),
            (mine, theirs),
        )
        first = shifted(hidden, dz=nl, cross=-1)
        second = shifted(hidden, dz=-nl, cross=-1)
        (mine,) = call(
            stack_kernel, (sds((nh, *hidden.shape), bf16),), (hidden, first, second)
        )
        labels = label_rows[None]
        while labels.shape[0] < ny:
            size = labels.shape[0]
            arrived = shifted(labels, dy=size)
            (labels,) = call(
                join_kernel,
                (sds((2 * size, own_count, columns), bf16),),
                (labels, arrived),
            )
        others = shifted(mine, dc=1)
        (by_x,) = call(
            functools.partial(down_kernel, nh),
            (sds((nx, nl * SLOTS, columns), bf16),),
            (mine, others, w_down),
            flops=2 * hidden.shape[0] * w_down.shape[1] * columns,
        )
        by_x = exchange(by_x, "x")
        (by_zl,) = call(sum_kernel, (sds((nl, SLOTS, columns), bf16),), (by_x,))
        by_zl, labels = lax.optimization_barrier((by_zl, labels))
        by_zl = exchange(by_zl, "zl")
        (sent,) = call(
            mix_kernel,
            (sds((ny, own_count, columns + LANES), bf16),),
            (by_zl, place, gate, labels, seg_ids, residual, label_rows),
            scratch=[pltpu.VMEM((count, LANES), f32)],
        )
        terms = exchange(sent, "y")
        (score,) = call(
            functools.partial(score_kernel, columns),
            (sds((nh * nc, 1, LANES), f32),),
            (terms,),
        )
        scores = exchange(score, TENSOR)
        (layer_out,) = call(
            out_kernel, (sds((own_count, columns), bf16),), (terms, residual)
        )
        (margins,) = call(
            margin_kernel, (sds((1, PAIRS), f32),), (scores, pair_slot, ref_scores)
        )
        return (layer_out, margins)

    return body


def solution(mesh):
    sizes = (4, 4, mesh.shape["expert"], 3, 2)
    fine = Mesh(mesh.devices.reshape(sizes), AXES)
    placed = (
        P(DP, None),
        P(),
        P(DP, None),
        P(DP, None),
        P("y", None, (*DP, *TENSOR)),
        P("y", None, (*DP, *TENSOR)),
        P("y", DP, TENSOR),
        P((*DP, "y"), TENSOR),
        P(DP, None),
        P(DP, None),
        P(DP, None),
    )
    return jax.shard_map(
        make_body(sizes),
        mesh=fine,
        in_specs=placed,
        out_specs=(P((*DP, "y"), TENSOR), P(DP, None)),
        check_vma=False,
    )
```

```python
import functools

import jax
import jax.numpy as jnp
from jax import lax
from jax.experimental import pallas as pl
from jax.experimental.pallas import tpu as pltpu
from jax.sharding import Mesh, PartitionSpec as P

SEQS = 4
PAIRS = 2
SLOTS = 36
LANES = 128
epsilon = 1e-05
dpo_beta = 0.5

AXES = ("x", "zl", "y", "zh", "c")
DP = ("x", "zl")
TENSOR = ("zh", "c")
OFFSETS = (0, 2, -1, 1)


f32 = jnp.float32
bf16 = jnp.bfloat16
VMEM = pl.BlockSpec(memory_space=pltpu.VMEM)
HBM = pl.BlockSpec(memory_space=pltpu.HBM)


def shift_pairs(sizes, dx=0, dy=0, dz=0, dc=0, cross=1):
    nx, nl, ny, nh, nc = sizes
    nz = nh * nl

    def flat(x, y, z, c):
        return (((x * nl + z % nl) * ny + y) * nh + z // nl) * nc + c

    pairs = []
    for x in range(nx):
        for y in range(ny):
            for z in range(nz):
                for c in range(nc):
                    way = cross if c else 1
                    target = flat(
                        (x + way * dx) % nx,
                        (y + dy) % ny,
                        (z + way * dz) % nz,
                        (c + dc) % nc,
                    )
                    pairs.append((flat(x, y, z, c), target))
    return pairs


def exchange(array, axis):
    return lax.all_to_all(array, axis, 0, 0, tiled=True)


def call(kernel, outs, ins, flops=0, in_specs=None, scratch=(), spare=4):
    size = sum(a.size * a.dtype.itemsize for a in (*ins, *outs))
    limit = min(size + (spare << 20), 60 << 20)
    return pl.pallas_call(
        kernel,
        out_shape=outs,
        in_specs=in_specs or [VMEM] * len(ins),
        out_specs=tuple(VMEM for _ in outs),
        scratch_shapes=list(scratch),
        compiler_params=pltpu.CompilerParams(vmem_limit_bytes=limit),
        cost_estimate=pl.CostEstimate(
            flops=flops or size, bytes_accessed=size, transcendentals=0
        ),
    )(*ins)


def column(row):
    return jnp.transpose(jnp.broadcast_to(row, (LANES, LANES)))


def front_kernel(own_count, columns, *refs):
    *ins, own_ref, far_ref, place_ref, gate_ref, res_ref, tok_ref, gain_ref, ids_ref, gw_ref, sems = refs
    count, width = tok_ref.shape
    quarter = width // 4
    small = [
        pltpu.make_async_copy(ref, held, sems.at[i])
        for i, (ref, held) in enumerate(
            zip(ins[1:], (gain_ref, ids_ref, gw_ref), strict=True)
        )
    ]
    large = [
        pltpu.make_async_copy(
            ins[0].at[:, pl.ds(i * quarter, quarter)],
            tok_ref.at[:, pl.ds(i * quarter, quarter)],
            sems.at[3 + i],
        )
        for i in range(4)
    ]
    for copy in small[1:] + large + small[:1]:
        copy.start()
    for copy in small[1:]:
        copy.wait()
    expert = lax.axis_index("y")
    core = lax.axis_index("c")
    step = 512
    match = ids_ref[...] == expert
    hit = match.astype(f32)
    named = hit[0:1] + hit[1:2]
    gate_row = jnp.sum(jnp.where(match, gw_ref[...], 0.0), axis=0, keepdims=True)
    gate_ref[...] = column(gate_row)
    before = lax.broadcasted_iota(jnp.int32, (count, count), 0)
    after = lax.broadcasted_iota(jnp.int32, (count, count), 1)
    position = jnp.dot(
        jnp.broadcast_to(named, (8, count)).astype(bf16),
        (before < after).astype(bf16),
        preferred_element_type=f32,
    )[0:1]
    slot = lax.broadcasted_iota(jnp.int32, (2 * SLOTS, count), 0).astype(f32)
    here = named > 0.5
    upper = jnp.where((slot == position) & here, 1.0, 0.0).astype(bf16)
    lower = jnp.where((slot - SLOTS == position) & here, 1.0, 0.0).astype(bf16)
    place_ref[...] = upper
    squares = jnp.zeros((count, step), f32)
    for start in range(0, width, step):
        if start % quarter == 0:
            large[start // quarter].wait()
        v = tok_ref[:, start : start + step].astype(f32)
        squares = squares + v * v
    total = jnp.sum(squares, axis=1, keepdims=True)
    inverse_rms = lax.rsqrt(total * (1.0 / width) + epsilon)
    small[0].wait()
    fold = own_ref.shape[2]
    half = 2 * fold
    nc = width // half
    column_at = (lax.axis_index("zh") * nc + core) * columns
    res_ref[...] = tok_ref[
        pl.ds(pl.multiple_of(expert * own_count, own_count), own_count),
        pl.ds(pl.multiple_of(column_at, LANES), columns),
    ]

    def normed(start):
        at = pl.multiple_of(core * half + start, LANES)
        v = tok_ref[:, pl.ds(at, step)].astype(f32)
        return (v * inverse_rms * gain_ref[:, pl.ds(at, step)]).astype(bf16)

    for start in range(0, fold, step):
        rows = jnp.dot(upper, normed(start), preferred_element_type=f32)
        rows += jnp.dot(lower, normed(start + fold), preferred_element_type=f32)
        rows = rows.astype(bf16)
        for x in range(own_ref.shape[0]):
            own_ref[x, :, start : start + step] = rows
        far_ref[:, start : start + step] = rows


def copies_kernel(in_ref, out_ref):
    for x in range(out_ref.shape[0]):
        out_ref[x] = in_ref[...]


def pack_kernel(in_ref, out_ref):
    blocks, folded, fold = in_ref.shape
    rows = out_ref.shape[0]
    step = 512
    to = lax.broadcasted_iota(jnp.int32, (rows, blocks * folded), 0)
    source = lax.broadcasted_iota(jnp.int32, (rows, blocks * folded), 1)
    for side in range(2):
        at = jnp.where(source < 0, 0, -1)
        for x in range(blocks):
            base = x * folded + side * SLOTS
            inside = (source >= base) & (source < base + SLOTS)
            at = jnp.where(inside, source - base + x * SLOTS, at)
        chosen = jnp.where(at == to, 1.0, 0.0).astype(bf16)
        for start in range(0, fold, step):
            block = jnp.concatenate(
                [in_ref[x, :, start : start + step] for x in range(blocks)], axis=0
            )
            moved = jnp.dot(chosen, block, preferred_element_type=f32).astype(bf16)
            out_ref[:, side * fold + start : side * fold + start + step] = moved


def slice_kernel(gate_ref, up_ref, send_ref, keep_ref, sems):
    half = send_ref.shape[1]
    core = lax.axis_index("c")
    copies = []
    for i, ref in enumerate((gate_ref, up_ref)):
        for j, (out, c) in enumerate(((send_ref, 1 - core), (keep_ref, core))):
            at = pl.multiple_of(c * half, 8)
            copies.append(
                pltpu.make_async_copy(
                    ref.at[0, pl.ds(at, half)], out.at[i], sems.at[2 * i + j]
                )
            )
    for copy in copies:
        copy.start()
    for copy in copies:
        copy.wait()


def dots_kernel(a_ref, b_ref, w_ref, *refs):
    *first, out_ref, sum_ref = refs
    rows, half = a_ref.shape
    step = 512
    sum_ref[...] = jnp.zeros_like(sum_ref)

    def body(k, _):
        at = pl.multiple_of(k * step, step)
        x = jnp.concatenate(
            [a_ref[:, pl.ds(at, step)], b_ref[:, pl.ds(at, step)]], axis=0
        )
        w = jnp.concatenate(
            [w_ref[0, pl.ds(at, step), :], w_ref[1, pl.ds(at, step), :]], axis=1
        )
        sum_ref[...] += jnp.dot(x, w, preferred_element_type=f32)
        return 0

    lax.fori_loop(0, half // step, body, 0)
    at = 0
    for ref in first:
        out_ref[at : at + ref.shape[0]] = ref[...]
        at += ref.shape[0]
    if not first:
        out_ref[...] = sum_ref[...]
        return
    core = lax.axis_index("c")
    for i in range(2):
        to = pl.multiple_of(at + lax.rem(core + i, 2) * rows, 16)
        out_ref[pl.ds(to, rows), :] = sum_ref[i * rows : (i + 1) * rows]


def dots(a, b, w, *first):
    rows, half = a.shape
    wide = 2 * w.shape[2]
    out = jax.ShapeDtypeStruct((2 * rows + sum(p.shape[0] for p in first), wide), f32)
    (sums,) = call(
        dots_kernel,
        (out,),
        (a, b, w, *first),
        flops=2 * 2 * rows * half * wide,
        scratch=[pltpu.VMEM((2 * rows, wide), f32)],
    )
    return sums


def hidden_kernel(nx, mine_ref, theirs_ref, out_ref):
    total, units = out_ref.shape
    block = total // nx
    parts = []
    for start in range(0, total, block):
        sums = mine_ref[start : start + block] + theirs_ref[start : start + block]
        gate, up = sums[:, :units], sums[:, units:]
        parts.append((gate / (1.0 + jnp.exp(-gate)) * up).astype(bf16))
    hidden = jnp.concatenate(parts, axis=0)
    slot = lax.broadcasted_iota(jnp.int32, (block, total), 0)
    source = lax.broadcasted_iota(jnp.int32, (block, total), 1)
    for x in range(nx):
        at = jnp.where(source < 0, 0, -1)
        for r in range(total // block):
            base = r * block + x * SLOTS
            inside = (source >= base) & (source < base + SLOTS)
            at = jnp.where(inside, source - base + r * SLOTS, at)
        chosen = jnp.where(at == slot, 1.0, 0.0).astype(bf16)
        moved = jnp.dot(chosen, hidden, preferred_element_type=f32)
        out_ref[x * block : (x + 1) * block] = moved.astype(bf16)


def stack_kernel(own_ref, first_ref, second_ref, out_ref):
    core = lax.axis_index("c")
    out_ref[0] = own_ref[...]
    out_ref[2 - core] = first_ref[...]
    out_ref[1 + core] = second_ref[...]


def down_kernel(nh, mine_ref, other_ref, w_ref, out_ref):
    nx, rows, _ = out_ref.shape
    units = mine_ref.shape[2]
    zh = lax.axis_index("zh")
    core = lax.axis_index("c")
    weights = []
    for step in range(nh):
        base = lax.rem(zh + step, nh) * 2
        weights.append(
            jnp.concatenate(
                [
                    w_ref[0, pl.ds(pl.multiple_of((base + c) * units, units), units), :]
                    for c in (core, 1 - core)
                ],
                axis=0,
            )
        )
    for x in range(nx):
        part = pl.ds(x * rows, rows)
        total = 0.0
        for step in range(nh):
            block = jnp.concatenate(
                [mine_ref[step, part, :], other_ref[step, part, :]], axis=1
            )
            total = total + jnp.dot(block, weights[step], preferred_element_type=f32)
        out_ref[x] = total.astype(bf16)


def sum_kernel(in_ref, out_ref):
    nl, slots, _ = out_ref.shape
    rows = in_ref.shape[1]
    zl = lax.axis_index("zl")
    total = in_ref[0].astype(f32)
    for i in range(1, in_ref.shape[0]):
        total = total + in_ref[i].astype(f32)
    total = total.astype(bf16)
    slot = lax.broadcasted_iota(jnp.int32, (slots, rows), 0)
    source = lax.broadcasted_iota(jnp.int32, (slots, rows), 1)
    for r, offset in enumerate(OFFSETS):
        chosen = jnp.where(source == slot + r * SLOTS, 1.0, 0.0).astype(bf16)
        moved = jnp.dot(chosen, total, preferred_element_type=f32)
        out_ref[lax.rem(zl + offset + nl, nl)] = moved.astype(bf16)


def join_kernel(a_ref, b_ref, out_ref):
    size = a_ref.shape[0]
    out_ref[:size] = a_ref[...]
    out_ref[size:] = b_ref[...]


def mix_kernel(in_ref, place_ref, gate_ref, labels_ref, seg_ref, res_ref, own_ref, out_ref, score_ref):
    ny, own_count, _ = out_ref.shape
    count, columns = ny * own_count, labels_ref.shape[2]
    expert = lax.axis_index("y")
    total = in_ref[0].astype(f32)
    for i in range(1, in_ref.shape[0]):
        total = total + in_ref[i].astype(f32)
    rows = jnp.concatenate(
        [
            total.astype(bf16),
            jnp.zeros((place_ref.shape[0] - total.shape[0], columns), bf16),
        ],
        axis=0,
    )
    picked = lax.dot_general(
        place_ref[...], rows, (((0,), (0,)), ((), ())), preferred_element_type=f32
    )
    weighted = (gate_ref[:, 0:1] * picked).astype(bf16)
    for y in range(ny):
        rows = slice(y * own_count, (y + 1) * own_count)
        label = labels_ref[lax.rem(expert - y + ny, ny)].astype(f32)
        row_score = jnp.sum(
            weighted[rows].astype(f32) * label, axis=1, keepdims=True
        )
        score_ref[rows, :] = jnp.broadcast_to(row_score, (own_count, LANES))
    own = jnp.sum(
        res_ref[...].astype(f32) * own_ref[...].astype(f32), axis=1, keepdims=True
    )
    at = pl.ds(pl.multiple_of(expert * own_count, own_count), own_count)
    score_ref[at, :] = score_ref[at, :] + jnp.broadcast_to(own, (own_count, LANES))
    sequence = column(seg_ref[...].astype(f32))
    lane = lax.broadcasted_iota(jnp.int32, (count, LANES), 1).astype(f32)
    member = jnp.where(sequence == lane, score_ref[...], 0.0)
    score = jnp.sum(member, axis=0, keepdims=True)
    first = score.astype(bf16).astype(f32)
    second = (score - first).astype(bf16).astype(f32)
    third = score - first - second
    row = lax.broadcasted_iota(jnp.int32, (own_count, LANES), 0)
    pads = jnp.where(
        row == 0,
        first,
        jnp.where(row == 1, second, jnp.where(row == 2, third, 0.0)),
    ).astype(bf16)
    for y in range(ny):
        out_ref[y, :, :columns] = weighted[y * own_count : (y + 1) * own_count]
        out_ref[y, :, columns:] = pads


def score_kernel(columns, in_ref, score_ref):
    total = in_ref[0, :, columns:].astype(f32)
    for y in range(1, in_ref.shape[0]):
        total = total + in_ref[y, :, columns:].astype(f32)
    score = jnp.sum(total, axis=0, keepdims=True)
    for i in range(score_ref.shape[0]):
        score_ref[i] = score


def out_kernel(in_ref, res_ref, out_ref):
    columns = out_ref.shape[1]
    total = in_ref[0, :, :columns].astype(f32)
    for y in range(1, in_ref.shape[0]):
        total = total + in_ref[y, :, :columns].astype(f32)
    out_ref[...] = (res_ref[...].astype(f32) + total).astype(bf16)


def margin_kernel(in_ref, slot_ref, ref_ref, out_ref):
    total = in_ref[0]
    for i in range(1, in_ref.shape[0]):
        total = total + in_ref[i]
    slots = slot_ref[...]
    pair = lax.shift_right_logical(slots, 1)
    polarity = (1 - 2 * (slots - 2 * pair)).astype(f32)
    signed = polarity * (total[:, :SEQS] - ref_ref[...])
    sums = [
        jnp.sum(jnp.where(pair == p, signed, 0.0), axis=1, keepdims=True)
        for p in range(PAIRS)
    ]
    out_ref[...] = dpo_beta * jnp.concatenate(sums, axis=1)


def make_body(sizes):
    nx, nl, ny, nh, nc = sizes

    def shifted(array, **shift):
        return lax.ppermute(array, AXES, shift_pairs(sizes, **shift))

    def body(
        tokens,
        norm_gain,
        expert_ids,
        gate_weights,
        w_gate,
        w_up,
        w_down,
        label_rows,
        seg_ids,
        pair_slot,
        ref_scores,
    ):
        count, width = tokens.shape
        half = width // nc
        fold = half // 2
        columns = width // (nh * nc)
        own_count = count // ny
        units = w_gate.shape[2]
        sds = jax.ShapeDtypeStruct
        own, own_far, place, gate, residual = call(
            functools.partial(front_kernel, own_count, columns),
            (
                sds((nx, 2 * SLOTS, fold), bf16),
                sds((2 * SLOTS, fold), bf16),
                sds((2 * SLOTS, count), bf16),
                sds((count, LANES), f32),
                sds((own_count, columns), bf16),
            ),
            (tokens, norm_gain[None, :], expert_ids.T, gate_weights.T),
            in_specs=[HBM] * 4,
            scratch=[
                pltpu.VMEM((count, width), bf16),
                pltpu.VMEM((1, width), f32),
                pltpu.VMEM((2, count), jnp.int32),
                pltpu.VMEM((2, count), f32),
                pltpu.SemaphoreType.DMA((7,)),
            ],
            spare=60,
        )
        near = exchange(own, "x")
        far = shifted(own_far, dz=2)
        w_send, w_mine = call(
            slice_kernel,
            (sds((2, half, units), bf16),) * 2,
            (w_gate, w_up),
            in_specs=[HBM, HBM],
            scratch=[pltpu.SemaphoreType.DMA((4,))],
            spare=60,
        )
        w_other = shifted(w_send, dc=1)
        (near,) = call(pack_kernel, (sds((nx * SLOTS, half), bf16),), (near,))
        first = shifted(near, dz=1, cross=-1)
        second = shifted(near, dz=-1, cross=-1)
        (far,) = call(copies_kernel, (sds(own.shape, bf16),), (far,))
        far = exchange(far, "x")
        (far,) = call(pack_kernel, (sds((nx * SLOTS, half), bf16),), (far,))
        early_other = dots(near, far, w_other)
        early_mine = dots(near, far, w_mine)
        first, second, early_mine = lax.optimization_barrier(
            (first, second, early_mine)
        )
        other = dots(first, second, w_other, early_other)
        theirs = shifted(other, dc=1)
        mine = dots(first, second, w_mine, early_mine)
        (hidden,) = call(
            functools.partial(hidden_kernel, nx),
            (sds((nx * nl * SLOTS, units), bf16),),
            (mine, theirs),
        )
        first = shifted(hidden, dz=nl, cross=-1)
        second = shifted(hidden, dz=-nl, cross=-1)
        (mine,) = call(
            stack_kernel, (sds((nh, *hidden.shape), bf16),), (hidden, first, second)
        )
        labels = label_rows[None]
        while labels.shape[0] < ny:
            size = labels.shape[0]
            arrived = shifted(labels, dy=size)
            (labels,) = call(
                join_kernel,
                (sds((2 * size, own_count, columns), bf16),),
                (labels, arrived),
            )
        others = shifted(mine, dc=1)
        (by_x,) = call(
            functools.partial(down_kernel, nh),
            (sds((nx, nl * SLOTS, columns), bf16),),
            (mine, others, w_down),
            flops=2 * hidden.shape[0] * w_down.shape[1] * columns,
        )
        by_x = exchange(by_x, "x")
        (by_zl,) = call(sum_kernel, (sds((nl, SLOTS, columns), bf16),), (by_x,))
        by_zl, labels = lax.optimization_barrier((by_zl, labels))
        by_zl = exchange(by_zl, "zl")
        (sent,) = call(
            mix_kernel,
            (sds((ny, own_count, columns + LANES), bf16),),
            (by_zl, place, gate, labels, seg_ids, residual, label_rows),
            scratch=[pltpu.VMEM((count, LANES), f32)],
        )
        terms = exchange(sent, "y")
        (score,) = call(
            functools.partial(score_kernel, columns),
            (sds((nh * nc, 1, LANES), f32),),
            (terms,),
        )
        scores = exchange(score, TENSOR)
        (layer_out,) = call(
            out_kernel, (sds((own_count, columns), bf16),), (terms, residual)
        )
        (margins,) = call(
            margin_kernel, (sds((1, PAIRS), f32),), (scores, pair_slot, ref_scores)
        )
        return (layer_out, margins)

    return body


def solution(mesh):
    sizes = (4, 4, mesh.shape["expert"], 3, 2)
    fine = Mesh(mesh.devices.reshape(sizes), AXES)
    placed = (
        P(DP, None),
        P(),
        P(DP, None),
        P(DP, None),
        P("y", None, (*DP, *TENSOR)),
        P("y", None, (*DP, *TENSOR)),
        P("y", DP, TENSOR),
        P((*DP, "y"), TENSOR),
        P(DP, None),
        P(DP, None),
        P(DP, None),
    )
    return jax.shard_map(
        make_body(sizes),
        mesh=fine,
        in_specs=placed,
        out_specs=(P((*DP, "y"), TENSOR), P(DP, None)),
        check_vma=False,
    )
```
